32 devices in a mesh: dp: 16 (over z, x, core), section: 2 (over y).
Axes of the slice: x: 2, y: 2, z: 4, core: 2. Of those that a mesh axis runs over, the one named last changes fastest.
Arguments:
- samples: bfloat16 [128, 512], P('dp'), may hold values from -6 to 6
- targets: bfloat16 [128, 512], P('dp'), may hold values from -6 to 6
- jacobian_targets: bfloat16 [128, 128, 512], P('dp'), may hold values from -0.1796875 to 0.1796875
- directions: int32 [128, 128], P('dp'), may hold values from 0 to 511
- plan: int32 [16, 8], P('dp'), may hold values from 0 to 7, each once within a row
- weights: bfloat16 [2, 512, 8192], P('section'), may hold values from -1 to 1
Outputs:
- gradients: float32 [2, 512, 8192], P('section', 'dp')
The draws below stay inside these ranges and needn't reach their ends.
Inputs may be any that keep to these rules, and one draw needn't show every extreme that they name: `plan`: each row is a permutation of 0 to 7.
All inputs are finite; a program needn't handle non-finite values.
Results may differ from the reference program's by a relative error of at most 0.0034.
Values may be sent and summed in bfloat16 or wider, within the bound.
A program may use at most 128 MiB of HBM per device.

```python
import jax
import jax.numpy as jnp
from jax import lax

REDUCED = 512
WIDTH = 8192
TANGENTS = 128
MICRO = 4
BATCH = 1
POOL = 8
SAMPLES = 128
N_DP = 16


def draw_weights(key, part):
    scales = jnp.array([REDUCED ** (-0.5), WIDTH ** (-0.5)], jnp.float32)[:, None, None]
    base = jnp.clip(jax.random.normal(key, (2, REDUCED, WIDTH), jnp.float32), -4.0, 4.0)
    return (base * scales).astype(jnp.bfloat16)


def place_ends(values, own_key, smallest, largest):
    extent = values.shape
    index_at = [jax.random.randint(jax.random.fold_in(own_key, axis), (), 0, extent[axis]) for axis in range(len(extent))]
    values = values.at[tuple(index_at)].set(smallest)
    longest = extent.index(max(extent))
    index_at[longest] = (index_at[longest] + 1) % extent[longest]
    return values.at[tuple(index_at)].set(largest)


def raised(values, stream_key, source, target, parts, factor):
    owner, partner = [(jnp.arange(values.shape[dim]) // (values.shape[dim] // parts)).reshape([-1 if axis == dim else 1 for axis in range(values.ndim)]) for dim in (source, target)]
    chosen = jax.random.permutation(stream_key, parts)[partner]
    strong = (owner == chosen) | (owner == (partner + parts // 2) % parts)
    return jnp.where(strong, factor * values, values)


def levels(own_key, extent, split, low, largest):
    loudness = 1.0
    for axis_at, parts in split:
        heights = jax.random.uniform(jax.random.fold_in(jax.random.fold_in(own_key, 6), axis_at), (parts,), jnp.float32, low / len(split), largest / len(split))
        loudness = loudness * jnp.repeat(jnp.exp(heights), extent[axis_at] // parts).reshape((-1,) + (1,) * (len(extent) - 1 - axis_at))
    return loudness


def gaussian(stream_key, extent, spread, most, split=(), held_as=jnp.bfloat16):
    loudness = levels(stream_key, extent, split, -0.22, 0.18) if split else 1.0
    result = jax.random.normal(stream_key, extent, jnp.float32) * spread * loudness
    return jnp.minimum(jnp.maximum(result, -most), most).astype(held_as)


def gaussian_with(stream_key, extent, scale, bound, pieces, heavy, kind=jnp.bfloat16):
    entries = scale * jax.random.normal(stream_key, extent, jnp.float32)
    if pieces:
        entries = entries * levels(stream_key, extent, pieces, -0.22, 0.18)
    return jnp.clip(raised(entries, jax.random.fold_in(stream_key, 3), *heavy), -bound, bound).astype(kind)


def setup_inputs(seed: int = 0) -> dict:
    arg_keys = jax.random.split(jax.random.key(seed), 7)
    samples = gaussian_with(arg_keys[0], (SAMPLES, REDUCED), 1.0, 6.0, ((0, 16),), (0, 1, 16, 2.0))
    targets = gaussian_with(arg_keys[1], (SAMPLES, REDUCED), 1.0, 6.0, ((0, 16),), (0, 1, 16, 2.0))
    jacobian_targets = gaussian(arg_keys[2], (SAMPLES, TANGENTS, REDUCED), 0.03, 0.1796875, ((0, 16),))
    directions = place_ends(jax.random.randint(arg_keys[3], (SAMPLES, TANGENTS), 0, REDUCED), jax.random.fold_in(arg_keys[3], 1), 0, REDUCED - 1).astype(jnp.int32)
    plan = jax.vmap(lambda own: jax.random.permutation(own, POOL))(jax.random.split(arg_keys[4], N_DP)).reshape((N_DP, POOL)).astype(jnp.int32)
    weights = draw_weights(jax.random.fold_in(arg_keys[6], 71), 0)
    return dict(samples=samples, targets=targets, jacobian_targets=jacobian_targets, directions=directions, plan=plan, weights=weights)


jacobian_weight = 32.0


def contract_rows(left, right):
    return lax.dot_general(left, right, (((0,), (0,)), ((), ())), preferred_element_type=jnp.float32)


def against_rows(left, right):
    return lax.dot_general(left, right, (((1,), (1,)), ((), ())), preferred_element_type=jnp.float32)


def encoder_parts(inputs, chosen_dirs, w_first):
    linear = jnp.dot(inputs, w_first, preferred_element_type=jnp.float32)
    squash = jax.nn.sigmoid(linear)
    first_slope = squash * (1.0 + linear * (1.0 - squash))
    second_slope = squash * (1.0 - squash) * (2.0 + linear * (1.0 - 2.0 * squash))
    picked = jnp.take(w_first, chosen_dirs, axis=0)
    return linear, squash, first_slope, second_slope, picked


def encoder_forward(encoded):
    linear, squash, first_slope, second_slope, picked = encoded
    hidden = (linear * squash).astype(jnp.bfloat16)
    tangent = (first_slope[:, None, :] * picked.astype(jnp.float32)).astype(jnp.bfloat16)
    return hidden, tangent


def decoder(hidden, tangent, w_last, target_rows, jacobian_rows):
    columns = hidden.shape[1]
    flattened = tangent.reshape(-1, columns)
    output = against_rows(hidden, w_last)
    jacobian = against_rows(flattened, w_last)
    misfit = (output - target_rows.astype(jnp.float32)).astype(jnp.bfloat16)
    jac_misfit = (jacobian_weight * (jacobian - jacobian_rows.reshape(jacobian.shape).astype(jnp.float32))).astype(jnp.bfloat16)
    grad_last = contract_rows(misfit, hidden) + contract_rows(jac_misfit, flattened)
    cotangent = jnp.dot(misfit, w_last, preferred_element_type=jnp.float32).astype(jnp.bfloat16)
    cotangent_tangent = jnp.dot(jac_misfit, w_last, preferred_element_type=jnp.float32).astype(jnp.bfloat16)
    return grad_last, cotangent, cotangent_tangent.reshape(tangent.shape)


def encoder_backward(inputs, chosen_dirs, encoded, cotangent, cotangent_tangent, reduced):
    linear, squash, first_slope, second_slope, picked = encoded
    projected = jnp.sum(cotangent_tangent.astype(jnp.float32) * picked.astype(jnp.float32), axis=1)
    grad_pre = (cotangent.astype(jnp.float32) * first_slope + second_slope * projected).astype(jnp.bfloat16)
    grad_picked = (cotangent_tangent.astype(jnp.float32) * first_slope[:, None, :]).astype(jnp.bfloat16)
    columns = grad_pre.shape[1]
    onehot = (chosen_dirs.reshape(-1)[:, None] == jnp.arange(reduced, dtype=jnp.int32)[None, :]).astype(jnp.bfloat16)
    return contract_rows(inputs, grad_pre) + contract_rows(onehot, grad_picked.reshape(-1, columns))


def reference(samples, targets, jacobian_targets, directions, plan, weights):
    w_first = weights[0]
    w_last = weights[1]
    offsets = jnp.arange(N_DP, dtype=jnp.int32) * POOL
    picked_rows = (plan[:, :MICRO * BATCH].astype(jnp.int32) + offsets[:, None]).reshape(-1).astype(jnp.int32)

    def accumulate(carried, position):
        first_total, last_total = carried
        inputs = lax.dynamic_slice_in_dim(samples, position, 1, 0)
        chosen_dirs = lax.dynamic_slice_in_dim(directions, position, 1, 0)
        target_rows = lax.dynamic_slice_in_dim(targets, position, 1, 0)
        jacobian_rows = lax.dynamic_slice_in_dim(jacobian_targets, position, 1, 0)
        encoded = encoder_parts(inputs, chosen_dirs, w_first)
        hidden, tangent = encoder_forward(encoded)
        grad_last, cotangent, cotangent_tangent = decoder(hidden, tangent, w_last, target_rows, jacobian_rows)
        grad_first = encoder_backward(inputs, chosen_dirs, encoded, cotangent, cotangent_tangent, REDUCED)
        return (first_total + grad_first, last_total + grad_last), None

    cleared = jnp.zeros((REDUCED, WIDTH), jnp.float32)
    totals, unused = lax.scan(accumulate, (cleared, cleared), picked_rows)
    return jnp.stack([totals[0], totals[1]])
```

```python
import functools

import jax
import jax.numpy as jnp
from jax import lax
from jax.experimental import pallas as pl
from jax.experimental.pallas import tpu as pltpu
from jax.sharding import PartitionSpec as P

MICRO = 4
GROUP = 4
PAD = 16

jacobian_weight = 32.0

VMEM = pl.BlockSpec(memory_space=pltpu.VMEM)
ANY = pl.BlockSpec(memory_space=pl.ANY)


def place():
    dp, sec = lax.axis_index("dp"), lax.axis_index("section")
    g = lax.rem(dp, GROUP)
    return dp, sec, g, dp - g


def greet(peers):
    barrier = pltpu.get_barrier_semaphore()
    for dp, sec in peers:
        pl.semaphore_signal(barrier, inc=1, device_id={"dp": dp, "section": sec})
    pl.semaphore_wait(barrier, len(peers))


def remote(src, dst, send, recv, dp, sec):
    return pltpu.make_async_remote_copy(
        src_ref=src, dst_ref=dst, send_sem=send, recv_sem=recv,
        device_id={"dp": dp, "section": sec},
    )


def spread_kernel(n_sec, pack, weight, packs, both, psend, precv, wsend, wrecv, local):
    dp, sec, g, base = place()
    cols = both.shape[2]
    near = [(base + lax.rem(g + k, GROUP), sec) for k in range(1, GROUP)]
    far = [(dp, lax.rem(sec + k, n_sec)) for k in range(1, n_sec)]
    greet(near + far)

    def part(section):
        start = pl.multiple_of((section * GROUP + g) * cols, cols)
        return weight.at[0, :, pl.ds(start, cols)]

    copies = [
        remote(part(s), both.at[sec], wsend.at[k], wrecv.at[k], d, s)
        for k, (d, s) in enumerate(far)
    ]
    copies += [
        remote(pack, packs.at[g], psend.at[k], precv.at[k], d, s)
        for k, (d, s) in enumerate(near)
    ]
    for copy in copies:
        copy.start()
    own = pltpu.make_async_copy(part(sec), both.at[sec], local)
    own.start()
    packs[g] = pack[...]
    own.wait()
    for copy in copies:
        copy.wait()


def forward_kernel(spt, dirs, xs, both, act, picked_out, slopes, partial):
    tangents = dirs.shape[1] // spt
    reduced = both.shape[1]
    rows = dirs.shape[1]
    lanes = lax.broadcasted_iota(jnp.int32, (rows, reduced), 1)
    onehot = (dirs[0] == lanes).astype(jnp.float32).astype(jnp.bfloat16)
    picked = jnp.dot(onehot, both[0], preferred_element_type=jnp.float32)
    picked_out[0] = picked.astype(jnp.bfloat16)
    linear = jnp.dot(xs[0], both[0], preferred_element_type=jnp.float32)
    squash = jax.nn.sigmoid(linear)
    first = squash * (1.0 + linear * (1.0 - squash))
    second = squash * (1.0 - squash) * (2.0 + linear * (1.0 - 2.0 * squash))
    slopes[0, 0:PAD] = first
    slopes[0, PAD : 2 * PAD] = second
    for i in range(spt):
        lo = i * tangents
        act[0, lo : lo + tangents] = (first[i : i + 1] * picked[lo : lo + tangents]).astype(
            jnp.bfloat16
        )
    act[0, rows:] = (linear * squash).astype(jnp.bfloat16)
    partial[0] = lax.dot_general(
        act[0], both[1], (((1,), (1,)), ((), ())), preferred_element_type=jnp.float32
    ).astype(jnp.bfloat16)


def misfit_kernel(
    n_sec, tangent_rows, partial, target, misfit,
    first_in, sums, second_in, s1, r1, s2, r2, s3, r3, s4, r4,
):
    dp, sec, g, base = place()
    half = GROUP // 2
    quads = n_sec * half
    core = lax.rem(g, 2)
    q = sec * half + g // 2
    partner = (base + (g // 2) * 2 + (1 - core), sec)

    def quad(k):
        other = lax.rem(q + k, quads)
        return other // half, lax.rem(other, half)

    def device(k):
        s, h = quad(k)
        return base + h * 2 + core, s

    def block(k, c):
        s, h = quad(k)
        return s * GROUP + h * 2 + c

    greet([partner] + [device(k) for k in range(1, quads)])
    order = list(range(1, quads)) + [0]
    across = [
        remote(partial.at[block(k, 1 - core)], first_in.at[k], s1.at[k], r1.at[k], *partner)
        for k in range(quads)
    ]
    for k in order:
        across[k].start()
    out = [None] + [
        remote(sums.at[k - 1], second_in.at[k - 1], s2.at[k - 1], r2.at[k - 1], *device(k))
        for k in range(1, quads)
    ]
    for k in range(1, quads):
        across[k].wait_recv()
        sums[k - 1] = (
            partial[block(k, core)].astype(jnp.float32) + first_in[k].astype(jnp.float32)
        ).astype(jnp.bfloat16)
        out[k].start()
    across[0].wait_recv()
    for k in range(quads):
        across[k].wait_send()
    mine = block(0, core)
    for k in range(1, quads):
        out[k].wait_recv()
    total = partial[mine].astype(jnp.float32) + first_in[0].astype(jnp.float32)
    for k in range(1, quads):
        total = total + second_in[k - 1].astype(jnp.float32)
    row = lax.broadcasted_iota(jnp.int32, total.shape, 0)
    gain = jnp.where(row < tangent_rows, jacobian_weight, 1.0)
    misfit[mine] = (gain * (total - target[...].astype(jnp.float32))).astype(jnp.bfloat16)
    for k in range(1, quads):
        out[k].wait_send()
    gather = [
        remote(misfit.at[mine], misfit.at[mine], s3.at[k - 1], r3.at[k - 1], *device(k))
        for k in range(1, quads)
    ]
    for copy in gather:
        copy.start()
    passed = [remote(misfit.at[mine], misfit.at[mine], s4.at[0], r4.at[0], *partner)]
    passed[0].start()
    for k in range(1, quads):
        gather[k - 1].wait_recv()
        came = block(quads - k, core)
        copy = remote(misfit.at[came], misfit.at[came], s4.at[k], r4.at[k], *partner)
        copy.start()
        passed.append(copy)
    for copy in gather:
        copy.wait_send()
    for copy in passed:
        copy.wait()


def backward_kernel(
    spt, dirs, xs, both, act, picked, slopes, misfit, grads, total, pulled, chosen
):
    step = pl.program_id(0)
    rows = dirs.shape[1]
    tangents = rows // spt
    reduced = both.shape[1]
    over_rows = (((0,), (0,)), ((), ()))

    @pl.when(step == 0)
    def _():
        total[...] = jnp.zeros_like(total)

    total[1] += lax.dot_general(
        misfit[0], act[0], over_rows, preferred_element_type=jnp.float32
    )
    cotangent = jnp.dot(misfit[0], both[1], preferred_element_type=jnp.float32).astype(jnp.bfloat16)
    first = slopes[0, 0:PAD]
    second = slopes[0, PAD : 2 * PAD]
    tail_row = lax.broadcasted_iota(jnp.int32, first.shape, 0)
    projected = jnp.zeros_like(first)
    for i in range(spt):
        lo = i * tangents
        part = cotangent[lo : lo + tangents].astype(jnp.float32)
        line = jnp.sum(
            part * picked[0, lo : lo + tangents].astype(jnp.float32), axis=0, keepdims=True
        )
        projected = jnp.where(tail_row == i, line, projected)
        pulled[lo : lo + tangents] = (part * first[i : i + 1]).astype(jnp.bfloat16)
    pulled[rows:] = (
        cotangent[rows:].astype(jnp.float32) * first + second * projected
    ).astype(jnp.bfloat16)
    lanes = lax.broadcasted_iota(jnp.int32, (rows, reduced), 1)
    chosen[:rows] = (dirs[0] == lanes).astype(jnp.float32).astype(jnp.bfloat16)
    chosen[rows:] = xs[0]
    total[0] += lax.dot_general(
        chosen[...], pulled[...], over_rows, preferred_element_type=jnp.float32
    )

    @pl.when(step == pl.num_programs(0) - 1)
    def _():
        grads[...] = total[...].astype(jnp.bfloat16)


def reduce_kernel(n_sec, n_s, grads, out, arrived, total, s1, r1, s2, r2, local):
    dp, sec, g, base = place()
    s = dp // GROUP
    team = n_sec * GROUP
    t = sec * GROUP + g
    _, rows, cols = grads.shape
    rows = rows // n_s
    own_rows = rows // GROUP

    def rows_of(owner):
        return pl.ds(pl.multiple_of(owner * rows, rows), rows)

    def mate(k):
        other = lax.rem(t + k, team)
        return other // GROUP, lax.rem(other, GROUP)

    peers = [lax.rem(s + k, n_s) for k in range(1, n_s)]
    mates = [mate(k) for k in range(1, team)]
    greet([(p * GROUP + g, sec) for p in peers] + [(base + h, l) for l, h in mates])
    sums = [
        remote(
            grads.at[:, rows_of(p), :], arrived.at[k], s1.at[k], r1.at[k], p * GROUP + g, sec
        )
        for k, p in enumerate(peers)
    ]
    for copy in sums:
        copy.start()
    for copy in sums:
        copy.wait_recv()
    for layer in range(n_sec):
        for h in range(GROUP):
            start = pl.multiple_of(s * rows + h * own_rows, own_rows)
            value = grads[layer, pl.ds(start, own_rows), :].astype(jnp.float32)
            for k in range(n_s - 1):
                value = value + arrived[k, layer, h * own_rows : (h + 1) * own_rows, :].astype(
                    jnp.float32
                )
            total[layer * GROUP + h] = value
    for copy in sums:
        copy.wait_send()
    columns = out.at[:, pl.ds(pl.multiple_of(t * cols, cols), cols)]
    hand = [
        remote(total.at[l * GROUP + h], columns, s2.at[k], r2.at[k], base + h, l)
        for k, (l, h) in enumerate(mates)
    ]
    for copy in hand:
        copy.start()
    keep = pltpu.make_async_copy(total.at[t], columns, local)
    keep.start()
    keep.wait()
    for copy in hand:
        copy.wait()


def shards(n_dp, n_sec, samples, targets, jacobian_targets, directions, plan, weights):
    sec = lax.axis_index("section")
    _, reduced, width = weights.shape
    tangents = directions.shape[1]
    team = n_sec * GROUP
    cols = width // team
    n_s = n_dp // GROUP
    spt = MICRO // n_sec
    rows = spt * tangents
    high = rows + PAD
    dma = lambda n: pltpu.SemaphoreType.DMA((n,))
    f32, bf16 = jnp.float32, jnp.bfloat16
    shape = jax.ShapeDtypeStruct
    limit = 56 * 1024 * 1024

    slots = plan[0, :MICRO]
    pack = jnp.concatenate(
        [
            jnp.take(samples, slots, axis=0).astype(f32),
            jnp.take(directions, slots, axis=0).astype(f32),
        ],
        axis=1,
    )
    pack = jnp.pad(pack, ((0, 8 - MICRO), (0, 0)))
    packs, both = pl.pallas_call(
        functools.partial(spread_kernel, n_sec),
        out_shape=(
            shape((GROUP,) + pack.shape, f32),
            shape((n_sec, reduced, cols), bf16),
        ),
        in_specs=[VMEM, ANY],
        out_specs=(VMEM, VMEM),
        scratch_shapes=[dma(GROUP - 1), dma(GROUP - 1), dma(n_sec - 1), dma(n_sec - 1),
                        pltpu.SemaphoreType.DMA],
        compiler_params=pltpu.CompilerParams(
            collective_id=0, has_side_effects=True, vmem_limit_bytes=limit
        ),
        name="spread",
    )(pack, weights)
    packs = packs[:, :MICRO].reshape(GROUP, n_sec, spt, -1).transpose(1, 0, 2, 3)
    packs = packs.reshape(team, spt, -1)
    xs = jnp.pad(packs[..., :reduced].astype(bf16), ((0, 0), (0, PAD - spt), (0, 0)))
    dirs = packs[..., reduced:].astype(jnp.int32).reshape(team, rows, 1)

    per = lambda *s: pl.BlockSpec((1,) + s, lambda i: (i,) + (0,) * len(s))
    all_of = lambda *s: pl.BlockSpec(s, lambda i: (0,) * len(s))
    common = [per(rows, 1), per(PAD, reduced), all_of(n_sec, reduced, cols)]
    act, picked, slopes, partial = pl.pallas_call(
        functools.partial(forward_kernel, spt),
        grid=(team,),
        out_shape=(
            shape((team, high, cols), bf16),
            shape((team, rows, cols), bf16),
            shape((team, 2 * PAD, cols), f32),
            shape((team, high, reduced), bf16),
        ),
        in_specs=common,
        out_specs=(per(high, cols), per(rows, cols), per(2 * PAD, cols), per(high, reduced)),
        compiler_params=pltpu.CompilerParams(vmem_limit_bytes=limit),
        name="forward",
    )(dirs, xs, both)

    own = lax.dynamic_slice_in_dim(slots, sec * spt, spt)
    target = jnp.concatenate(
        [
            jnp.take(jacobian_targets, own, axis=0).reshape(rows, reduced),
            jnp.pad(jnp.take(targets, own, axis=0), ((0, PAD - spt), (0, 0))),
        ]
    )
    quads = team // 2
    misfit = pl.pallas_call(
        functools.partial(misfit_kernel, n_sec, rows),
        out_shape=shape((team, high, reduced), bf16),
        in_specs=[VMEM, VMEM],
        out_specs=VMEM,
        scratch_shapes=[
            pltpu.VMEM((quads, high, reduced), bf16),
            pltpu.VMEM((quads - 1, high, reduced), bf16),
            pltpu.VMEM((quads - 1, high, reduced), bf16),
            dma(quads), dma(quads), dma(quads - 1), dma(quads - 1),
            dma(quads - 1), dma(quads - 1), dma(quads), dma(quads),
        ],
        compiler_params=pltpu.CompilerParams(
            collective_id=1, has_side_effects=True, vmem_limit_bytes=limit
        ),
        name="misfit",
    )(partial, target)

    grads = pl.pallas_call(
        functools.partial(backward_kernel, spt),
        grid=(team,),
        out_shape=shape((n_sec, reduced, cols), bf16),
        in_specs=common
        + [per(high, cols), per(rows, cols), per(2 * PAD, cols), per(high, reduced)],
        out_specs=all_of(n_sec, reduced, cols),
        scratch_shapes=[
            pltpu.VMEM((n_sec, reduced, cols), f32),
            pltpu.VMEM((high, cols), bf16),
            pltpu.VMEM((high, reduced), bf16),
        ],
        compiler_params=pltpu.CompilerParams(vmem_limit_bytes=limit),
        name="backward",
    )(dirs, xs, both, act, picked, slopes, misfit)

    own_rows = reduced // n_dp
    result = pl.pallas_call(
        functools.partial(reduce_kernel, n_sec, n_s),
        out_shape=shape((own_rows, width), f32),
        in_specs=[VMEM],
        out_specs=VMEM,
        scratch_shapes=[
            pltpu.VMEM((n_s - 1, n_sec, reduced // n_s, cols), bf16),
            pltpu.VMEM((team, own_rows, cols), f32),
            dma(n_s - 1), dma(n_s - 1), dma(team - 1), dma(team - 1),
            pltpu.SemaphoreType.DMA,
        ],
        compiler_params=pltpu.CompilerParams(
            collective_id=2, has_side_effects=True, vmem_limit_bytes=limit
        ),
        name="reduce",
    )(grads)
    return result[None]


def solution(mesh):
    placed = (
        P("dp", None),
        P("dp", None),
        P("dp", None, None),
        P("dp", None),
        P("dp", None),
        P("section", None, None),
    )
    body = functools.partial(shards, mesh.shape["dp"], mesh.shape["section"])
    return jax.shard_map(
        body, mesh=mesh, in_specs=placed, out_specs=P("section", "dp", None), check_vma=False
    )
```

```python
import functools

import jax
import jax.numpy as jnp
from jax import lax
from jax.experimental import pallas as pl
from jax.experimental.pallas import tpu as pltpu
from jax.sharding import PartitionSpec as P

MICRO = 4
GROUP = 4
PAD = 16
PIECES = 4

jacobian_weight = 32.0

VMEM = pl.BlockSpec(memory_space=pltpu.VMEM)
ANY = pl.BlockSpec(memory_space=pl.ANY)


def place():
    dp, sec = lax.axis_index("dp"), lax.axis_index("section")
    g = lax.rem(dp, GROUP)
    return dp, sec, g, dp - g


def greet(peers):
    barrier = pltpu.get_barrier_semaphore()
    for dp, sec in peers:
        pl.semaphore_signal(barrier, inc=1, device_id={"dp": dp, "section": sec})
    pl.semaphore_wait(barrier, len(peers))


def remote(src, dst, send, recv, dp, sec):
    return pltpu.make_async_remote_copy(
        src_ref=src, dst_ref=dst, send_sem=send, recv_sem=recv,
        device_id={"dp": dp, "section": sec},
    )


def spread_kernel(
    n_sec, n_s, plan, samples, directions, weight, packs, both,
    psend, precv, wsend, wrecv, zsend, zrecv, local,
):
    dp, sec, g, base = place()
    _, reduced, cols = both.shape
    parity = lax.rem(dp // GROUP, 2)
    twin = (dp + GROUP * (1 - 2 * parity), sec)
    near = [(base + lax.rem(g + k, GROUP), sec) for k in range(1, GROUP)]
    far = [(dp, lax.rem(sec + k, n_sec)) for k in range(1, n_sec)]
    greet(near + far + [twin])
    piece = reduced // 2 // PIECES

    def part(section):
        start = pl.multiple_of((section * GROUP + g) * cols, cols)
        return weight.at[0, :, pl.ds(start, cols)]

    def rows_of(c):
        return pl.ds(pl.multiple_of(parity * (reduced // 2) + c * piece, piece), piece)

    sent = []
    for c in range(PIECES):
        for k, (d, s) in enumerate(far):
            i = k * PIECES + c
            sent.append(
                remote(
                    part(s).at[rows_of(c)], both.at[sec, rows_of(c)],
                    wsend.at[i], wrecv.at[i], d, s,
                )
            )
    for copy in sent:
        copy.start()
    own = pltpu.make_async_copy(part(sec), both.at[sec], local)
    own.start()
    every = jnp.concatenate(
        [samples[...].astype(jnp.float32), directions[...].astype(jnp.float32)], axis=1
    )
    row = lax.broadcasted_iota(jnp.int32, every.shape, 0)
    packed = jnp.zeros_like(every)
    for k in range(MICRO):
        line = jnp.sum(jnp.where(row == plan[0, k], every, 0.0), axis=0, keepdims=True)
        packed = jnp.where(row == k, line, packed)
    packs[g] = packed
    own.wait()
    shared = [
        remote(packs.at[g], packs.at[g], psend.at[k], precv.at[k], d, s)
        for k, (d, s) in enumerate(near)
    ]
    for copy in shared:
        copy.start()
    passed = []
    for c in range(PIECES):
        for k in range(n_sec - 1):
            i = k * PIECES + c
            sent[c * (n_sec - 1) + k].wait_recv()
            came = both.at[lax.rem(sec + n_sec - 1 - k, n_sec), rows_of(c)]
            copy = remote(came, came, zsend.at[i], zrecv.at[i], *twin)
            copy.start()
            passed.append(copy)
    for copy in shared + passed:
        copy.wait()
    for copy in sent:
        copy.wait_send()


def onehot_columns(directions_row, reduced):
    rows = lax.broadcasted_iota(jnp.int32, (reduced, directions_row.shape[1]), 0)
    return (rows == directions_row.astype(jnp.int32)).astype(jnp.float32).astype(jnp.bfloat16)


def stack_rows(lines, shape):
    row = lax.broadcasted_iota(jnp.int32, shape, 0)
    result = jnp.zeros(shape, jnp.float32)
    for i, line in enumerate(lines):
        result = jnp.where(row == i, line, result)
    return result


def pack_row(packs, block, spt, i):
    return packs[lax.rem(block, GROUP), pl.ds(block // GROUP * spt + i, 1), :]


def forward_kernel(
    spt, plan, sec, packs, both, jac_target, targets,
    act, picked_out, slopes, partial, jac_out, target_out,
):
    block = pl.program_id(0)
    tangents, reduced = jac_target.shape[1:]
    rows = spt * tangents
    jac_out[...] = jac_target[...]

    @pl.when(block == 0)
    def _():
        all_targets = targets[...].astype(jnp.float32)
        row = lax.broadcasted_iota(jnp.int32, all_targets.shape, 0)
        lines = [
            jnp.sum(
                jnp.where(row == plan[0, sec[0] * spt + i], all_targets, 0.0),
                axis=0, keepdims=True,
            )
            for i in range(spt)
        ]
        target_out[...] = stack_rows(lines, target_out.shape).astype(jnp.bfloat16)

    packed = [pack_row(packs, block, spt, i) for i in range(spt)]
    xs = stack_rows([p[:, :reduced] for p in packed], (PAD, reduced)).astype(jnp.bfloat16)
    linear = jnp.dot(xs, both[0], preferred_element_type=jnp.float32)
    squash = jax.nn.sigmoid(linear)
    first = squash * (1.0 + linear * (1.0 - squash))
    second = squash * (1.0 - squash) * (2.0 + linear * (1.0 - 2.0 * squash))
    slopes[0, 0:PAD] = first
    slopes[0, PAD : 2 * PAD] = second
    for i in range(spt):
        lo = i * tangents
        picked = lax.dot_general(
            onehot_columns(packed[i][:, reduced:], reduced), both[0],
            (((0,), (0,)), ((), ())), preferred_element_type=jnp.float32,
        )
        picked_out[0, lo : lo + tangents] = picked.astype(jnp.bfloat16)
        act[0, lo : lo + tangents] = (first[i : i + 1] * picked).astype(jnp.bfloat16)
    act[0, rows:] = (linear * squash).astype(jnp.bfloat16)
    partial[0] = lax.dot_general(
        act[0], both[1], (((1,), (1,)), ((), ())), preferred_element_type=jnp.float32
    ).astype(jnp.bfloat16)


def step_kernel(
    n_sec, n_s, spt,
    partial, jac_target, target, packs, both, act_hbm, picked_hbm, slopes_hbm, out,
    first_in, sums, second_in, misfit, act, picked, slopes, total, grads,
    tails, xs_all, inbox, halves, finished,
    s1, r1, s2, r2, s3, r3, s4, r4, s5, r5, s6, r6, load, local,
):
    dp, sec, g, base = place()
    s = dp // GROUP
    half = GROUP // 2
    team = n_sec * GROUP
    quads = n_sec * half
    core = lax.rem(g, 2)
    q = sec * half + g // 2
    partner = (base + (g // 2) * 2 + (1 - core), sec)
    rows, reduced = spt * jac_target.shape[1], both.shape[1]
    tangents = rows // spt
    cols = both.shape[2]
    slab = reduced // n_s
    own_rows = slab // GROUP
    f32, bf16 = jnp.float32, jnp.bfloat16
    over_rows = (((0,), (0,)), ((), ()))

    def quad(k):
        other = lax.rem(q + k, quads)
        return other // half, lax.rem(other, half)

    def device(k):
        l, h = quad(k)
        return base + h * 2 + core, l

    def block(k, c):
        l, h = quad(k)
        return l * GROUP + h * 2 + c

    if n_s == 4:
        mate = s + 1 - 2 * lax.rem(s, 2)
        opposite = lax.rem(s + 2, 4)
        mate_opposite = lax.rem(mate + 2, 4)
        others = [mate, opposite]
    else:
        others = [lax.rem(s + k, n_s) for k in range(1, n_s)]
    team_peers = [
        ((base + lax.rem(g + k, GROUP)), lax.rem(sec + j, n_sec))
        for j in range(n_sec) for k in range(GROUP) if j or k
    ]
    greet(team_peers + [(o * GROUP + g, sec) for o in others])
    loads = [
        pltpu.make_async_copy(a, b, load.at[i])
        for i, (a, b) in enumerate(((act_hbm, act), (picked_hbm, picked), (slopes_hbm, slopes)))
    ]

    across = [
        remote(partial.at[block(k, 1 - core)], first_in.at[k], s1.at[k], r1.at[k], *partner)
        for k in range(quads)
    ]
    for k in list(range(1, quads)) + [0]:
        across[k].start()
    for copy in loads:
        copy.start()
    away = [None] + [
        remote(sums.at[k - 1], second_in.at[k - 1], s2.at[k - 1], r2.at[k - 1], *device(k))
        for k in range(1, quads)
    ]
    for k in range(1, quads):
        across[k].wait_recv()
        sums[k - 1] = (
            partial[block(k, core)].astype(f32) + first_in[k].astype(f32)
        ).astype(bf16)
        away[k].start()
    across[0].wait_recv()
    for k in range(quads):
        across[k].wait_send()
    mine = block(0, core)
    for k in range(1, quads):
        away[k].wait_recv()

    def whole(lo, hi):
        value = partial[mine, lo:hi].astype(f32) + first_in[0, lo:hi].astype(f32)
        for k in range(1, quads):
            value = value + second_in[k - 1, lo:hi].astype(f32)
        return value

    for i in range(spt):
        lo, hi = i * tangents, (i + 1) * tangents
        misfit[mine, lo:hi] = (
            jacobian_weight * (whole(lo, hi) - jac_target[i].astype(f32))
        ).astype(bf16)
    misfit[mine, rows:] = (whole(rows, rows + PAD) - target[...].astype(f32)).astype(bf16)
    for k in range(1, quads):
        away[k].wait_send()
    gather = [
        remote(misfit.at[mine], misfit.at[mine], s3.at[k - 1], r3.at[k - 1], *device(k))
        for k in range(1, quads)
    ]
    for copy in gather:
        copy.start()
    passed = [remote(misfit.at[mine], misfit.at[mine], s4.at[0], r4.at[0], *partner)]
    passed[0].start()
    for copy in loads:
        copy.wait()

    def last_of(b):
        total[1] += lax.dot_general(misfit[b], act[b], over_rows, preferred_element_type=f32)

    total[...] = jnp.zeros_like(total)
    last_of(mine)
    passed[0].wait_recv()
    last_of(block(0, 1 - core))
    for k in range(1, quads):
        gather[k - 1].wait_recv()
        came = block(quads - k, core)
        copy = remote(misfit.at[came], misfit.at[came], s4.at[k], r4.at[k], *partner)
        copy.start()
        passed.append(copy)
        last_of(came)
    for k in range(1, quads):
        passed[k].wait_recv()
        last_of(block(quads - k, 1 - core))

    def slab_of(owner):
        return pl.ds(pl.multiple_of(owner * slab, slab), slab)

    def link(layer, kind, source, to):
        i = layer * inbox.shape[1] + kind
        return remote(source, inbox.at[layer, kind], s5.at[i], r5.at[i], to * GROUP + g, sec)

    flights = {}

    def send_layer(layer):
        grads[layer] = total[layer].astype(bf16)
        if n_s == 4:
            flights[layer] = [
                link(layer, 0, grads.at[layer, slab_of(mate_opposite)], mate),
                link(layer, 1, grads.at[layer, slab_of(mate)], mate),
            ]
        else:
            flights[layer] = [
                link(layer, k, grads.at[layer, slab_of(o)], o) for k, o in enumerate(others)
            ]
        for copy in flights[layer]:
            copy.start()

    def relay(layer):
        if n_s == 4:
            flights[layer][0].wait_recv()
            halves[layer] = (
                grads[layer, slab_of(opposite), :].astype(f32) + inbox[layer, 0].astype(f32)
            ).astype(bf16)
            copy = link(layer, 2, halves.at[layer], opposite)
            copy.start()
            flights[layer].append(copy)

    columns = out.at[:, pl.ds(pl.multiple_of((sec * GROUP + g) * cols, cols), cols)]

    def hand(layer, k):
        h = lax.rem(g + k, GROUP)
        return remote(
            finished.at[layer * GROUP + h], columns,
            s6.at[layer * GROUP + k], r6.at[sec * GROUP + k], base + h, layer,
        )

    def keep():
        return pltpu.make_async_copy(finished.at[sec * GROUP + g], columns, local)

    def finish(layer):
        kinds = range(1, 3) if n_s == 4 else range(n_s - 1)
        for k in kinds:
            flights[layer][k].wait_recv()
        for h in range(GROUP):
            start = pl.multiple_of(s * slab + h * own_rows, own_rows)
            value = grads[layer, pl.ds(start, own_rows), :].astype(f32)
            for k in kinds:
                value = value + inbox[layer, k, h * own_rows : (h + 1) * own_rows].astype(f32)
            finished[layer * GROUP + h] = value
        for copy in flights[layer]:
            copy.wait_send()
        for k in range(1, GROUP):
            hand(layer, k).start()

        @pl.when(sec != layer)
        def _():
            hand(layer, 0).start()

        @pl.when(sec == layer)
        def _():
            keep().start()

    def pull(b, carry):
        cotangent = jnp.dot(misfit[b], both[1], preferred_element_type=f32)
        first = slopes[b, 0:PAD]
        second = slopes[b, PAD : 2 * PAD]
        lines = []
        chosen = []
        pulled = []
        packed = [pack_row(packs, b, spt, i) for i in range(spt)]
        for i in range(spt):
            lo = i * tangents
            part = cotangent[lo : lo + tangents]
            lines.append(
                jnp.sum(part * picked[b, lo : lo + tangents].astype(f32), axis=0, keepdims=True)
            )
            pulled.append((part * first[i : i + 1]).astype(bf16))
            chosen.append(onehot_columns(packed[i][:, reduced:], reduced))
        here = pl.ds(pl.multiple_of(b * PAD, PAD), PAD)
        tails[here, :] = (
            cotangent[rows:] * first + second * stack_rows(lines, first.shape)
        ).astype(bf16)
        xs_all[here, :] = stack_rows([p[:, :reduced] for p in packed], (PAD, reduced)).astype(bf16)
        total[0] += jnp.dot(
            jnp.concatenate(chosen, axis=1), jnp.concatenate(pulled, axis=0),
            preferred_element_type=f32,
        )
        return carry

    send_layer(1)
    lax.fori_loop(0, team // 2, pull, 0)
    relay(1)
    lax.fori_loop(team // 2, team, pull, 0)
    total[0] += lax.dot_general(
        xs_all[...], tails[...], over_rows, preferred_element_type=f32
    )
    send_layer(0)
    finish(1)
    relay(0)
    finish(0)

    for layer in range(n_sec):
        for k in range(1, GROUP):
            hand(layer, k).wait_send()

        @pl.when(sec != layer)
        def _():
            hand(layer, 0).wait_send()

    keep().wait()
    for j in range(n_sec):
        for k in range(GROUP):
            arrival = remote(
                finished.at[0], columns, s6.at[0], r6.at[j * GROUP + k], *partner
            )
            if k:
                arrival.wait_recv()
            else:

                @pl.when(sec != j)
                def _():
                    arrival.wait_recv()

    for copy in gather + passed:
        copy.wait_send()


def shards(n_dp, n_sec, samples, targets, jacobian_targets, directions, plan, weights):
    sec = lax.axis_index("section")
    _, reduced, width = weights.shape
    pool, tangents = directions.shape
    team = n_sec * GROUP
    cols = width // team
    n_s = n_dp // GROUP
    spt = MICRO // n_sec
    rows = spt * tangents
    high = rows + PAD
    dma = lambda n: pltpu.SemaphoreType.DMA((n,))
    f32, bf16 = jnp.float32, jnp.bfloat16
    shape = jax.ShapeDtypeStruct
    limit = 56 * 1024 * 1024

    links = (n_sec - 1) * PIECES
    packs, both = pl.pallas_call(
        functools.partial(spread_kernel, n_sec, n_s),
        out_shape=(
            shape((GROUP, pool, reduced + tangents), f32),
            shape((n_sec, reduced, cols), bf16),
        ),
        in_specs=[pl.BlockSpec(memory_space=pltpu.SMEM), VMEM, VMEM, ANY],
        out_specs=(VMEM, VMEM),
        scratch_shapes=[dma(GROUP - 1), dma(GROUP - 1), dma(links), dma(links),
                        dma(links), dma(links), pltpu.SemaphoreType.DMA],
        compiler_params=pltpu.CompilerParams(
            collective_id=0, has_side_effects=True, vmem_limit_bytes=limit
        ),
        name="spread",
    )(plan, samples, directions, weights)

    per = lambda *s: pl.BlockSpec((1,) + s, lambda i, *_: (i,) + (0,) * len(s))
    all_of = lambda *s: pl.BlockSpec(s, lambda i, *_: (0,) * len(s))
    sample = lambda i: jnp.minimum(i, spt - 1)
    act, picked, slopes, partial, jac_target, target = pl.pallas_call(
        functools.partial(forward_kernel, spt),
        out_shape=(
            shape((team, high, cols), bf16),
            shape((team, rows, cols), bf16),
            shape((team, 2 * PAD, cols), f32),
            shape((team, high, reduced), bf16),
            shape((spt, tangents, reduced), bf16),
            shape((PAD, reduced), bf16),
        ),
        grid_spec=pltpu.PrefetchScalarGridSpec(
            num_scalar_prefetch=2,
            grid=(team,),
            in_specs=[
                all_of(*packs.shape),
                all_of(*both.shape),
                pl.BlockSpec(
                    (1, tangents, reduced),
                    lambda i, plan, sec: (plan[0, sec[0] * spt + sample(i)], 0, 0),
                ),
                all_of(*targets.shape),
            ],
            out_specs=(
                per(high, cols), per(rows, cols), per(2 * PAD, cols), per(high, reduced),
                pl.BlockSpec((1, tangents, reduced), lambda i, *_: (sample(i), 0, 0)),
                all_of(PAD, reduced),
            ),
        ),
        compiler_params=pltpu.CompilerParams(vmem_limit_bytes=limit),
        name="forward",
    )(plan, sec.reshape(1), packs, both, jacobian_targets, targets)

    quads = team // 2
    kinds = 3 if n_s == 4 else n_s - 1
    slab = reduced // n_s
    vmem = pltpu.VMEM
    result = pl.pallas_call(
        functools.partial(step_kernel, n_sec, n_s, spt),
        out_shape=shape((reduced // n_dp, width), f32),
        in_specs=[VMEM] * 5 + [ANY] * 3,
        out_specs=VMEM,
        scratch_shapes=[
            vmem((quads, high, reduced), bf16),
            vmem((quads - 1, high, reduced), bf16),
            vmem((quads - 1, high, reduced), bf16),
            vmem((team, high, reduced), bf16),
            vmem(act.shape, bf16),
            vmem(picked.shape, bf16),
            vmem(slopes.shape, f32),
            vmem((n_sec, reduced, cols), f32),
            vmem((n_sec, reduced, cols), bf16),
            vmem((team * PAD, cols), bf16),
            vmem((team * PAD, reduced), bf16),
            vmem((n_sec, kinds, slab, cols), bf16),
            vmem((n_sec, slab, cols), bf16),
            vmem((team, reduced // n_dp, cols), f32),
            dma(quads), dma(quads), dma(quads - 1), dma(quads - 1),
            dma(quads - 1), dma(quads - 1), dma(quads), dma(quads),
            dma(n_sec * kinds), dma(n_sec * kinds), dma(team), dma(team),
            dma(3), pltpu.SemaphoreType.DMA,
        ],
        compiler_params=pltpu.CompilerParams(
            collective_id=1, has_side_effects=True, vmem_limit_bytes=limit
        ),
        name="step",
    )(partial, jac_target, target, packs, both, act, picked, slopes)
    return result[None]


def solution(mesh):
    placed = (
        P("dp", None),
        P("dp", None),
        P("dp", None, None),
        P("dp", None),
        P("dp", None),
        P("section", None, None),
    )
    body = functools.partial(shards, mesh.shape["dp"], mesh.shape["section"])
    return jax.shard_map(
        body, mesh=mesh, in_specs=placed, out_specs=P("section", "dp", None), check_vma=False
    )
```
